32 devices in a mesh: row: 8 (over y, x, core), col: 4 (over z).
Axes of the slice: x: 2, y: 2, z: 4, core: 2. Of those that a mesh axis runs over, the one named last changes fastest.
Arguments:
- hidden_in: bfloat16 [1152, 2048], P('col', 'row'), may hold values from -21 to 21
- state: float32 [128, 2048, 1152], P('col', 'row'), may hold values from -4 to 4
- attn_norm_gain: bfloat16 [2048], replicated, may hold values from 0.099609375 to 1.8984375
- w_query: bfloat16 [2048, 2048], P(None, 'row'), may hold values from -0.125 to 0.125
- w_key: bfloat16 [2048, 2048], P(None, 'row'), may hold values from -0.125 to 0.125
- w_value: bfloat16 [2048, 2048], P(None, 'row'), may hold values from -0.125 to 0.125
- w_gate: bfloat16 [2048, 2048], P(None, 'row'), may hold values from -0.125 to 0.125
- w_decay: bfloat16 [2048, 16], replicated, may hold values from -0.125 to 0.125
- w_beta: bfloat16 [2048, 16], replicated, may hold values from -0.125 to 0.125
- decay_log: float32 [16], replicated, may hold values from -3 to 1.5
- decay_bias: float32 [16], replicated, may hold values from -2 to 1
- head_gain: float32 [128], replicated, may hold values from 0.1 to 1.9
- w_out: bfloat16 [2048, 2048], P('row'), may hold values from -0.125 to 0.125
- final_gain: bfloat16 [2048], P('row'), may hold values from 0.099609375 to 1.8984375
- lm_weight: bfloat16 [2048, 20480], P(None, ('row', 'col')), may hold values from -0.28726213 to 0.28726213
- token_ids: int32 [1152], replicated, may hold values from 0 to 20479
- ref_logprob: float32 [1152], replicated, may hold values from -16 to -6
Outputs:
- new_state: float32 [128, 2048, 1152], P('col', 'row')
- logprob: float32 [1152], replicated
- entropy: float32 [1152], replicated
- kl: float32 [1152], replicated
The draws below stay inside these ranges and needn't reach their ends.
All inputs are finite; a program needn't handle non-finite values.
Results may differ from the reference program's by a relative error of at most 0.0014.
The reference program's roundings to bfloat16 on the way (of `normed`, `mixed_heads` and `final`) count: a program that leaves them out, or rounds other values in their place, can miss the bound.
Values may be sent and summed in bfloat16 or wider, within the bound.
A program may use at most 128 MiB of HBM per device.

```python
import jax
import jax.numpy as jnp
from jax import lax

D = 2048
HEADS = 16
DK = 128
DV = 128
VOCAB_DEV = 640
BATCH = 1152
VOCAB = 20480


def shared_sign(key):
    flips = jax.random.bernoulli(jax.random.fold_in(key, 101), 0.5, (D,))
    return jnp.where(flips, 1.0, -1.0).astype(jnp.float32)


def aligned_rows(key):
    level = jax.random.randint(jax.random.fold_in(key, 102), (BATCH,), 0, 3)
    chosen_rows = jnp.arange(BATCH, dtype=jnp.int32) % 5 == 0
    strength = 1.5 * jnp.exp2(level.astype(jnp.float32))
    return jnp.where(chosen_rows, strength, 0.0)


def draw_hidden_in(key, part):
    column_scale = 1.0 + 2.0 * jnp.arange(D, dtype=jnp.float32) / D
    strength = aligned_rows(key)
    base = jnp.clip(jax.random.normal(jax.random.fold_in(key, 3), (BATCH, D), jnp.float32), -4.0, 4.0)
    spread = base * column_scale[None, :]
    aligned = strength[:, None] * shared_sign(key)[None, :] + base
    values = jnp.where(strength[:, None] > 0.0, aligned, spread)
    return values.astype(jnp.bfloat16)


def draw_lm_weight(key, part):
    column_scale = 1.0 + 2.0 * jnp.arange(VOCAB, dtype=jnp.float32) / VOCAB
    base = jnp.clip(jax.random.normal(jax.random.fold_in(key, 6), (D, VOCAB), jnp.float32), -4.0, 4.0)
    base = base * column_scale[None, :] / jnp.sqrt(jnp.float32(D))
    chosen = jax.random.randint(jax.random.fold_in(key, 5), (4,), 0, VOCAB - 1)
    heights = (280.0 - 30.0 * jnp.arange(4, dtype=jnp.float32)) / jnp.float32(D)
    strength = jnp.zeros((VOCAB,), jnp.float32)
    strength = strength.at[chosen + 1].set(heights - 2.0 / jnp.float32(D))
    strength = strength.at[chosen].set(heights)
    values = jnp.where(strength[None, :] > 0.0, shared_sign(key)[:, None] * strength[None, :], base)
    return values.astype(jnp.bfloat16)


def plant(values, own_key, least, top_value):
    index_at = [jax.random.randint(jax.random.fold_in(own_key, axis), (), 0, length) for axis, length in enumerate(values.shape)]
    longest = values.shape.index(max(values.shape))
    next_to = index_at[:longest] + [(index_at[longest] + 1) % values.shape[longest]] + index_at[longest + 1:]
    return values.at[tuple(index_at)].set(least).at[tuple(next_to)].set(top_value)


def steps_of(key, shape, pieces, low, largest):
    factor_of, own = 1.0, jax.random.fold_in(key, 6)
    for dim, shards_of in pieces:
        draws = jnp.exp(jax.random.uniform(jax.random.fold_in(own, dim), (shards_of,), jnp.float32, low / len(pieces), largest / len(pieces)))
        factor_of = factor_of * jnp.repeat(draws, shape[dim] // shards_of).reshape([-1 if axis == dim else 1 for axis in range(len(shape))])
    return factor_of


def bell_draw(key, dims, scale, limit, cuts=(), kind=jnp.bfloat16):
    values = jax.random.normal(key, dims, jnp.float32) * scale
    if len(cuts) > 0:
        values = steps_of(key, dims, cuts, -0.22, 0.18) * values
    return jnp.clip(values, min=-limit, max=limit).astype(kind)


def setup_inputs(seed: int = 0) -> dict:
    keys = jax.random.split(jax.random.key(seed), 18)
    return {
        "hidden_in": draw_hidden_in(jax.random.fold_in(keys[17], 71), 0),
        "state": bell_draw(keys[1], (DK, HEADS * DV, BATCH), 0.5, 4.0, ((0, 4), (1, 8)), jnp.float32),
        "attn_norm_gain": jnp.clip(1.0 + 0.18 * jax.random.normal(keys[2], (D,), jnp.float32), 0.099609375, 1.8984375).astype(jnp.bfloat16),
        "w_query": bell_draw(keys[3], (D, HEADS * DK), D ** -0.5, 0.125, ((1, 8),)),
        "w_key": bell_draw(keys[4], (D, HEADS * DK), D ** -0.5, 0.125, ((1, 8),)),
        "w_value": bell_draw(keys[5], (D, HEADS * DV), D ** -0.5, 0.125, ((1, 8),)),
        "w_gate": bell_draw(keys[6], (D, HEADS * DV), D ** -0.5, 0.125, ((1, 8),)),
        "w_decay": bell_draw(keys[7], (D, HEADS), D ** -0.5, 0.125),
        "w_beta": bell_draw(keys[8], (D, HEADS), D ** -0.5, 0.125),
        "decay_log": jnp.clip(jax.random.uniform(keys[9], (HEADS,), jnp.float32, -3.0, 1.5), -3.0, 1.5),
        "decay_bias": jnp.clip(jax.random.uniform(keys[10], (HEADS,), jnp.float32, -2.0, 1.0), -2.0, 1.0),
        "head_gain": jnp.clip(1.0 + 0.18 * jax.random.normal(keys[11], (DV,), jnp.float32), 0.1, 1.9),
        "w_out": bell_draw(keys[12], (HEADS * DV, D), (HEADS * DV) ** -0.5, 0.125, ((0, 8),)),
        "final_gain": jnp.clip(1.0 + 0.18 * jax.random.normal(keys[13], (D,), jnp.float32), 0.099609375, 1.8984375).astype(jnp.bfloat16),
        "lm_weight": draw_lm_weight(jax.random.fold_in(keys[17], 71), 0),
        "token_ids": plant(jax.random.randint(keys[15], (BATCH,), 0, VOCAB), jax.random.fold_in(keys[15], 1), 0, VOCAB - 1).astype(jnp.int32),
        "ref_logprob": jnp.clip(jax.random.uniform(keys[16], (BATCH,), jnp.float32, -16.0, -6.0), -16.0, -6.0),
    }


def reference(hidden_in, state, attn_norm_gain, w_query, w_key, w_value, w_gate, w_decay, w_beta, decay_log, decay_bias, head_gain, w_out, final_gain, lm_weight, token_ids, ref_logprob):
    highest = lax.Precision.HIGHEST
    x = hidden_in.astype(jnp.float32)
    normed = (x * lax.rsqrt(lax.optimization_barrier(jnp.mean(x * x, axis=1, keepdims=True)) + 1e-06) * attn_norm_gain.astype(jnp.float32)).astype(jnp.bfloat16)
    qraw = lax.optimization_barrier(jnp.dot(normed, w_query, preferred_element_type=jnp.float32).astype(jnp.bfloat16)).astype(jnp.float32).reshape(BATCH, HEADS, DK)
    kraw = lax.optimization_barrier(jnp.dot(normed, w_key, preferred_element_type=jnp.float32).astype(jnp.bfloat16)).astype(jnp.float32).reshape(BATCH, HEADS, DK)
    query = (qraw * lax.rsqrt(lax.optimization_barrier(jnp.sum(qraw * qraw, axis=2, keepdims=True)) + 1e-06)).astype(jnp.bfloat16).astype(jnp.float32)
    key = (kraw * lax.rsqrt(lax.optimization_barrier(jnp.sum(kraw * kraw, axis=2, keepdims=True)) + 1e-06)).astype(jnp.bfloat16).astype(jnp.float32)
    value = jnp.dot(normed, w_value, preferred_element_type=jnp.float32).reshape(BATCH, HEADS, DV)
    gate = jnp.dot(normed, w_gate, preferred_element_type=jnp.float32).reshape(BATCH, HEADS, DV)
    decay_in = jnp.dot(normed, w_decay, preferred_element_type=jnp.float32)
    alpha = jnp.exp(-jnp.exp(decay_log)[None, :] * jax.nn.softplus(decay_in + decay_bias[None, :]))
    beta = jax.nn.sigmoid(jnp.dot(normed, w_beta, preferred_element_type=jnp.float32))
    alpha_t = alpha.T
    beta_t = beta.T
    tiles = state.reshape(DK, HEADS, DV, BATCH)
    recall = jnp.einsum('khvb,bhk->hvb', tiles, key, precision=highest)
    value_t = jnp.transpose(value, (1, 2, 0))
    write = beta_t[:, None, :] * (value_t - alpha_t[:, None, :] * recall)
    key_t = jnp.transpose(key, (2, 1, 0))
    updated = alpha_t[None, :, None, :] * tiles + key_t[:, :, None, :] * write[None]
    readout = jnp.einsum('khvb,bhk->hvb', updated, query, precision=highest)
    power = lax.optimization_barrier(jnp.mean(readout * readout, axis=1, keepdims=True))
    gate_t = jnp.transpose(gate, (1, 2, 0))
    mixed = readout * lax.rsqrt(power + 1e-05) * head_gain[None, :, None] * jax.nn.silu(gate_t)
    mixed_heads = jnp.transpose(mixed, (2, 0, 1)).reshape(BATCH, HEADS * DV).astype(jnp.bfloat16)
    hidden = x + jnp.dot(mixed_heads, w_out, preferred_element_type=jnp.float32)
    final = (hidden * lax.rsqrt(lax.optimization_barrier(jnp.mean(hidden * hidden, axis=1, keepdims=True)) + 1e-06) * final_gain.astype(jnp.float32)).astype(jnp.bfloat16)
    shards = VOCAB // VOCAB_DEV
    columns = jnp.arange(VOCAB_DEV, dtype=jnp.int32)

    def shard_step(index, carry):
        top, total, weighted, picked = carry
        piece = lax.dynamic_slice_in_dim(lm_weight, (index * VOCAB_DEV).astype(jnp.int32), VOCAB_DEV, 1)
        logits = jnp.dot(final, piece, preferred_element_type=jnp.float32)
        local_top = lax.optimization_barrier(jnp.max(logits, axis=1))
        new_top = jnp.maximum(top, local_top)
        shrink = jnp.exp(top - new_top)
        expo = jnp.exp(logits - new_top[:, None])
        total = total * shrink + lax.optimization_barrier(jnp.sum(expo, axis=1))
        weighted = weighted * shrink + lax.optimization_barrier(jnp.sum(expo * logits, axis=1))
        hits = columns[None, :] + (index * VOCAB_DEV).astype(jnp.int32) == token_ids[:, None]
        picked = picked + lax.optimization_barrier(jnp.sum(jnp.where(hits, logits, jnp.zeros_like(logits)), axis=1))
        return (new_top, total, weighted, picked)
    start = (jnp.full((BATCH,), -1e+30, jnp.float32), jnp.zeros((BATCH,), jnp.float32), jnp.zeros((BATCH,), jnp.float32), jnp.zeros((BATCH,), jnp.float32))
    top, total, weighted, picked = lax.fori_loop(jnp.int32(0), jnp.int32(shards), shard_step, start)
    lse = top + jnp.log(total)
    logprob = picked - lse
    entropy = lse - weighted / total
    gap = jnp.clip(ref_logprob - logprob, -20.0, 20.0)
    kl = jnp.minimum(jnp.exp(gap) - gap - 1.0, 10.0)
    new_state = updated.reshape(DK, HEADS * DV, BATCH)
    return (new_state, logprob, entropy, kl)
```

```python
import functools

import jax
import jax.numpy as jnp
from jax import lax
from jax.experimental import pallas as pl
from jax.experimental.pallas import tpu as pltpu
from jax.sharding import PartitionSpec as P

D = 2048
HEADS = 16
DK = 128
DV = 128
LANES = 128


def partner_2(block, axis, apart):
    count = lax.axis_size(axis)
    route = []
    for low in range(count):
        high = low | 1 << apart
        if high != low and high < count:
            route += [(low, high), (high, low)]
    return lax.ppermute(block, axis, route)


def project(weight, normed):
    return lax.dot_general(
        weight, normed, (((0,), (1,)), ((), ())), preferred_element_type=jnp.float32
    )


def shift_pairs(count, step):
    return [(source, (source + step) % count) for source in range(count)]


def swap_blocks(blocks, axis):
    count = lax.axis_size(axis)
    me = lax.axis_index(axis)
    result = blocks
    for step in range(1, count):
        sent = lax.dynamic_index_in_dim(blocks, (me + step) % count, 0, keepdims=True)
        got = lax.ppermute(sent, axis, shift_pairs(count, step))
        result = lax.dynamic_update_slice_in_dim(result, got, (me - step) % count, 0)
    return result


def gather_blocks(block, axis):
    count = lax.axis_size(axis)
    me = lax.axis_index(axis)
    result = jnp.zeros((count,) + block.shape, block.dtype)
    result = lax.dynamic_update_slice_in_dim(result, block[None], me, 0)
    for step in range(1, count):
        got = lax.ppermute(block[None], axis, shift_pairs(count, step))
        result = lax.dynamic_update_slice_in_dim(result, got, (me - step) % count, 0)
    return result


def sum_blocks(blocks, axis):
    count = lax.axis_size(axis)
    me = lax.axis_index(axis)
    total = lax.dynamic_index_in_dim(blocks, me, 0, keepdims=False)
    for step in range(1, count):
        sent = lax.dynamic_index_in_dim(blocks, (me + step) % count, 0, keepdims=False)
        total = total + lax.ppermute(sent, axis, shift_pairs(count, step))
    return total


def merge_stats(stats, axis):
    every = lax.all_gather(stats, axis, axis=0, tiled=False)
    top = jnp.max(every[:, 0], axis=0)
    shrink = jnp.exp(every[:, 0] - top[None])
    return jnp.stack(
        [
            top,
            jnp.sum(every[:, 1] * shrink, axis=0),
            jnp.sum(every[:, 2] * shrink, axis=0),
            jnp.sum(every[:, 3], axis=0),
        ]
    )


def per_device(
    hidden_in,
    state,
    attn_norm_gain,
    w_query,
    w_key,
    w_value,
    w_gate,
    w_decay,
    w_beta,
    decay_log,
    decay_bias,
    head_gain,
    w_out,
    final_gain,
    lm_weight,
    token_ids,
    ref_logprob,
):
    highest = lax.Precision.HIGHEST
    row_count = lax.axis_size("row")
    col_count = lax.axis_size("col")
    row_index = lax.axis_index("row")
    col_index = lax.axis_index("col")
    group = max(1, row_count // HEADS)
    local_heads = max(1, HEADS // row_count)
    first_head = row_index // group * local_heads
    value_cols = w_value.shape[1]
    value_part = value_cols // local_heads
    block_rows = hidden_in.shape[0]
    key_rows = state.shape[0]
    batch = state.shape[2]
    vocab_dev = lm_weight.shape[1]
    packed = jnp.concatenate([hidden_in, final_gain[None, :]], axis=0)
    whole = lax.all_gather(packed, "row", axis=1, tiled=True)
    whole_rows = whole[:block_rows]
    whole_gain = whole[block_rows].astype(jnp.float32)
    xfull = whole_rows.astype(jnp.float32)
    normed = (
        xfull
        * lax.rsqrt(jnp.mean(xfull * xfull, axis=1, keepdims=True) + 1e-06)
        * attn_norm_gain.astype(jnp.float32)
    ).astype(jnp.bfloat16)
    raw_pair = jnp.stack([project(w_query, normed), project(w_key, normed)]).astype(jnp.bfloat16)
    raw_pair = lax.optimization_barrier(raw_pair)
    for level in range(group.bit_length() - 1):
        partner = partner_2(raw_pair, "row", level)
        upper = row_index >> level & 1 == 1
        raw_pair = jnp.where(
            upper,
            jnp.concatenate([partner, raw_pair], axis=1),
            jnp.concatenate([raw_pair, partner], axis=1),
        )
    pair_f = raw_pair.astype(jnp.float32).reshape(2, local_heads, DK, block_rows)
    unit_pair = (
        pair_f * lax.rsqrt(jnp.sum(pair_f * pair_f, axis=2, keepdims=True) + 1e-06)
    ).astype(jnp.bfloat16)
    key_blocks = unit_pair.reshape(2, local_heads, col_count, key_rows, block_rows)
    swapped = swap_blocks(jnp.transpose(key_blocks, (2, 0, 1, 3, 4)), "col")
    tiles_qk = jnp.transpose(swapped, (1, 2, 3, 0, 4)).reshape(2, local_heads, key_rows, batch)
    query = tiles_qk[0].astype(jnp.float32)
    key = tiles_qk[1].astype(jnp.float32)
    unit_f = unit_pair.astype(jnp.float32)
    intersection = jnp.sum(unit_f[0] * unit_f[1], axis=1)
    value_t = project(w_value, normed)
    gate_t = project(w_gate, normed)
    decay_in = lax.dynamic_slice_in_dim(project(w_decay, normed), first_head, local_heads, 0)
    beta_in = lax.dynamic_slice_in_dim(project(w_beta, normed), first_head, local_heads, 0)
    rate = jnp.exp(lax.dynamic_slice_in_dim(decay_log, first_head, local_heads, 0))
    bias = lax.dynamic_slice_in_dim(decay_bias, first_head, local_heads, 0)
    alpha_t = jnp.exp(-rate[:, None] * jax.nn.softplus(decay_in + bias[:, None]))
    beta_t = jax.nn.sigmoid(beta_in)
    tiles = state.reshape(key_rows, local_heads, value_part, batch)
    value4 = value_t.reshape(local_heads, value_part, block_rows)
    key_major = jnp.transpose(key, (1, 0, 2))
    responses = jnp.stack(
        [
            jnp.einsum("khvb,hkb->hvb", tiles, key, precision=highest),
            jnp.einsum("khvb,hkb->hvb", tiles, query, precision=highest),
        ]
    )
    responses = responses.reshape(2, local_heads, value_part, col_count, block_rows)
    recall, answer = lax.psum_scatter(jnp.transpose(responses, (3, 0, 1, 2, 4)), "col", scatter_dimension=0, tiled=False)
    write = beta_t[:, None, :] * (value4 - alpha_t[:, None, :] * recall)
    parts = gather_blocks(
        jnp.concatenate([write.reshape(value_cols, block_rows), alpha_t], axis=0), "col"
    )
    parts = jnp.transpose(parts, (1, 0, 2)).reshape(value_cols + local_heads, batch)
    write_all = parts[:value_cols].reshape(local_heads, value_part, batch)
    alpha_all = parts[value_cols:]
    updated = alpha_all[None, :, None, :] * tiles + key_major[:, :, None, :] * write_all[None]
    readout = alpha_t[:, None, :] * answer + intersection[:, None, :] * write
    power = jnp.sum(readout * readout, axis=1)
    for level in range(group.bit_length() - 1):
        power = power + partner_2(power, "row", level)
    gain_part = lax.dynamic_slice_in_dim(head_gain, row_index % group * value_part, value_part, 0)
    gate4 = gate_t.reshape(local_heads, value_part, block_rows)
    mixed = (
        readout
        * lax.rsqrt(power / DV + 1e-05)[:, None, :]
        * gain_part[None, :, None]
        * jax.nn.silu(gate4)
    )
    mixed_heads = mixed.reshape(value_cols, block_rows).astype(jnp.bfloat16)
    share = -(-block_rows // row_count)
    extra = share * row_count - block_rows
    partial = lax.dot_general(
        mixed_heads, w_out, (((0,), (0,)), ((), ())), preferred_element_type=jnp.float32
    )
    branch = lax.psum_scatter(
        jnp.pad(partial, ((0, extra), (0, 0))).reshape(row_count, share, D),
        "row",
        scatter_dimension=0,
        tiled=False,
    )
    own_rows = lax.dynamic_slice_in_dim(
        jnp.pad(whole_rows, ((0, extra), (0, 0))), row_index * share, share, 0
    )
    hidden = own_rows.astype(jnp.float32) + branch
    energy = jnp.mean(hidden * hidden, axis=1, keepdims=True)
    final = (hidden * lax.rsqrt(energy + 1e-06) * whole_gain[None, :]).astype(jnp.bfloat16)
    tall = lax.all_gather(final, ("col", "row"), axis=0, tiled=True)
    if extra:
        tall = tall.reshape(col_count, share * row_count, D)[:, :block_rows].reshape(batch, D)
    logits = jnp.dot(tall, lm_weight, preferred_element_type=jnp.float32)
    vocab_start = (row_index * col_count + col_index) * vocab_dev
    hits = jnp.arange(vocab_dev, dtype=jnp.int32)[None, :] + vocab_start == token_ids[:, None]
    local_pick = jnp.sum(jnp.where(hits, logits, jnp.zeros_like(logits)), axis=1)
    local_top = jnp.max(logits, axis=1)
    expo = jnp.exp(logits - local_top[:, None])
    local_total = jnp.sum(expo, axis=1)
    local_weighted = jnp.sum(expo * logits, axis=1)
    stats = jnp.stack([local_top, local_total, local_weighted, local_pick])
    top, total, weighted, picked = merge_stats(merge_stats(stats, "col"), "row")
    lse = top + jnp.log(total)
    logprob = picked - lse
    entropy = lse - weighted / total
    gap = jnp.clip(ref_logprob - logprob, -20.0, 20.0)
    kl = jnp.minimum(jnp.exp(gap) - gap - 1.0, 10.0)
    new_state = updated.reshape(key_rows, value_cols, batch)
    return (new_state, logprob, entropy, kl)


MESH_IDS = pl.DeviceIdType.MESH


def remote(src, dst, send_sem, recv_sem, device):
    return pltpu.make_async_remote_copy(
        src_ref=src, dst_ref=dst, send_sem=send_sem, recv_sem=recv_sem,
        device_id=device, device_id_type=MESH_IDS,
    )


def meet(peers):
    barrier = pltpu.get_barrier_semaphore()
    for peer in peers:
        pl.semaphore_signal(barrier, inc=1, device_id=peer, device_id_type=MESH_IDS)
    pl.semaphore_wait(barrier, len(peers))


def places(rows, cols):
    me_r, me_c = lax.axis_index("row"), lax.axis_index("col")
    mate = me_r + 1 - 2 * lax.rem(me_r, 2)
    return me_r, me_c, mate


def all_peers(rows, cols):
    me_r, me_c, _ = places(rows, cols)
    peers = [(lax.rem(me_r + step, rows), me_c) for step in range(1, rows)]
    return peers + [(me_r, lax.rem(me_c + step, cols)) for step in range(1, cols)]


def row_gather_start(slots, rows, cols, send, recv):
    me_r, me_c, mate = places(rows, cols)
    chips = rows // 2
    copies = []
    for j in range(1, chips):
        peer = lax.rem(me_r + 2 * j, rows)
        copies.append(remote(slots.at[me_r], slots.at[me_r], send.at[j], recv.at[j], (peer, me_c)))
    own = remote(slots.at[me_r], slots.at[me_r], send.at[0], recv.at[0], (mate, me_c))
    for copy in copies:
        copy.start()
    own.start()
    return own, copies


def row_gather_finish(slots, rows, cols, send, recv, own, copies):
    me_r, me_c, mate = places(rows, cols)
    chips = rows // 2
    passed = []
    for j in range(1, chips):
        copies[j - 1].wait_recv()
        source = lax.rem(me_r + rows - 2 * j, rows)
        copy = remote(
            slots.at[source], slots.at[source], send.at[chips + j], recv.at[chips + j], (mate, me_c)
        )
        copy.start()
        passed.append(copy)
    own.wait_recv()
    for copy in passed:
        copy.wait_recv()
    for copy in [own] + copies + passed:
        copy.wait_send()


def first_kernel(
    rows, cols, heads, key_rows,
    hid, gain, w4_hbm, w5_hbm, w6_hbm, w7_hbm, w_decay, w_beta, decay_log, decay_bias,
    qk_out, value_out, gate_out, scal_out, alpha_out,
    xg, normed, weights, blocks, w_sem, row_send, row_recv, col_send, col_recv, a_send, a_recv,
):
    me_r, me_c, mate = places(rows, cols)
    count, width = hid.shape
    loads = []
    for index, source in enumerate((w4_hbm, w5_hbm, w6_hbm, w7_hbm)):
        load = pltpu.make_async_copy(source, weights.at[index], w_sem.at[index])
        load.start()
        loads.append(load)
    xg[me_r] = hid[...]
    meet(all_peers(rows, cols))
    own, copies = row_gather_start(xg, rows, cols, row_send, row_recv)
    row_gather_finish(xg, rows, cols, row_send, row_recv, own, copies)
    power = jnp.zeros((count, 1), jnp.float32)
    for r in range(rows):
        block = xg[r].astype(jnp.float32)
        power = power + jnp.sum(block * block, axis=1, keepdims=True)
    scale = lax.rsqrt(power / (rows * width) + 1e-06)
    for r in range(rows):
        block = xg[r].astype(jnp.float32)
        normed[:, r * width:(r + 1) * width] = (
            block * scale * gain[r * width:(r + 1) * width][None, :].astype(jnp.float32)
        ).astype(jnp.bfloat16)
    units, products = [], []
    for index in range(2):
        loads[index].wait()
        raw = jnp.dot(normed[...], weights[index], preferred_element_type=jnp.float32)
        raw = raw.astype(jnp.bfloat16).astype(jnp.float32)
        for h in range(heads):
            part = raw[:, h * DK:(h + 1) * DK]
            unit = part * lax.rsqrt(jnp.sum(part * part, axis=1, keepdims=True) + 1e-06)
            units.append(unit.astype(jnp.bfloat16))
    line = 2 * heads * key_rows
    total = 2 * heads * DK
    given = lax.broadcasted_iota(jnp.int32, (total, total), 0)
    taken = lax.broadcasted_iota(jnp.int32, (total, total), 1)
    inside = lax.rem(taken, line)
    wanted = inside // key_rows * DK + taken // line * key_rows + lax.rem(inside, key_rows)
    select = jnp.where(given == wanted, 1.0, 0.0).astype(jnp.bfloat16)
    packed = jnp.dot(
        jnp.concatenate(units, axis=1), select, preferred_element_type=jnp.float32
    ).astype(jnp.bfloat16)
    for c in range(cols):
        blocks[c] = packed[:, c * line:(c + 1) * line]
    qk_copies = []
    for step in range(1, cols):
        peer = lax.rem(me_c + step, cols)
        copy = remote(blocks.at[peer], qk_out.at[me_c], col_send.at[step], col_recv.at[step], (me_r, peer))
        copy.start()
        qk_copies.append(copy)
    qk_out[me_c] = blocks[me_c]
    over = (((1,), (1,)), ((), ()))
    decay_in = lax.dot_general(normed[...], w_decay[...], over, preferred_element_type=jnp.float32)
    beta_in = lax.dot_general(normed[...], w_beta[...], over, preferred_element_type=jnp.float32)
    z = decay_in + decay_bias[...]
    soft = jnp.maximum(z, 0.0) + jnp.log1p(jnp.exp(-jnp.abs(z)))
    alpha16 = jnp.exp(-jnp.exp(decay_log[...]) * soft)
    beta16 = 1.0 / (1.0 + jnp.exp(-beta_in))
    column = lax.broadcasted_iota(jnp.int32, alpha16.shape, 1)
    lane = lax.broadcasted_iota(jnp.int32, scal_out.shape, 1)
    scal = jnp.zeros(scal_out.shape, jnp.float32)
    for h in range(heads):
        mine = column == me_r * heads + h
        alpha = jnp.sum(jnp.where(mine, alpha16, 0.0), axis=1, keepdims=True)
        beta = jnp.sum(jnp.where(mine, beta16, 0.0), axis=1, keepdims=True)
        inter = jnp.sum(
            units[h].astype(jnp.float32) * units[heads + h].astype(jnp.float32), axis=1, keepdims=True
        )
        scal = jnp.where(lane == h, alpha, scal)
        scal = jnp.where(lane == heads + h, beta, scal)
        scal = jnp.where(lane == 2 * heads + h, inter, scal)
    scal_out[...] = scal
    alpha_out[me_c] = jnp.transpose(scal)[0:8, :]
    a_copies = []
    for step in range(1, cols):
        peer = lax.rem(me_c + step, cols)
        copy = remote(alpha_out.at[me_c], alpha_out.at[me_c], a_send.at[step], a_recv.at[step], (me_r, peer))
        copy.start()
        a_copies.append(copy)
    loads[2].wait()
    value_out[...] = jnp.dot(normed[...], weights[2], preferred_element_type=jnp.float32)
    loads[3].wait()
    gate_out[...] = jnp.dot(normed[...], weights[3], preferred_element_type=jnp.float32)
    for copy in qk_copies + a_copies:
        copy.wait()


def response_kernel(heads, key_rows, tile, cols, state, qk, recall_out, answer_out, key_out, qk_t, acc):
    step = pl.program_id(0)
    per_head = DV // tile
    batch = state.shape[2]
    count = batch // cols
    h = step // per_head

    @pl.when(step == 0)
    def _():
        for c in range(batch // LANES):
            part = qk[c * LANES:(c + 1) * LANES, :].astype(jnp.float32)
            qk_t[:, c * LANES:(c + 1) * LANES] = jnp.transpose(part)
        key_out[...] = qk_t[heads * key_rows:, :]

    v0 = pl.multiple_of(lax.rem(step, per_head) * tile, tile)
    q0 = pl.multiple_of(h * key_rows, key_rows)
    k0 = pl.multiple_of((heads + h) * key_rows, key_rows)

    def lanes_step(c, _):
        lanes = pl.ds(pl.multiple_of(c * LANES, LANES), LANES)
        keys = qk_t[pl.ds(k0, key_rows), lanes]
        queries = qk_t[pl.ds(q0, key_rows), lanes]
        recall = jnp.zeros((tile, LANES), jnp.float32)
        answer = jnp.zeros((tile, LANES), jnp.float32)
        for k in range(key_rows):
            cell = state[k, :, lanes]
            recall = recall + cell * keys[k:k + 1]
            answer = answer + cell * queries[k:k + 1]
        acc[0, pl.ds(v0, tile), lanes] = recall
        acc[1, pl.ds(v0, tile), lanes] = answer
        return 0

    lax.fori_loop(0, batch // LANES, lanes_step, 0)

    @pl.when(lax.rem(step, per_head) == per_head - 1)
    def _():
        head = pl.ds(pl.multiple_of(h * DV, DV), DV)
        for t, out in enumerate((recall_out, answer_out)):
            flat = jnp.transpose(acc[t]).astype(out.dtype)
            for c in range(cols):
                out[c, :, head] = flat[c * count:(c + 1) * count, :]


def update_kernel(heads, key_rows, tile, state, key, alpha, write, out, write_t, alpha_t):
    step = pl.program_id(0)
    per_head = DV // tile
    batch = state.shape[2]
    h = step // per_head

    @pl.when(step == 0)
    def _():
        for c in range(batch // LANES):
            part = write[c * LANES:(c + 1) * LANES, :].astype(jnp.float32)
            write_t[:, c * LANES:(c + 1) * LANES] = jnp.transpose(part)
        every = jnp.concatenate([alpha[c] for c in range(alpha.shape[0])], axis=1)
        for n in range(heads):
            alpha_t[8 * n:8 * n + 8, :] = jnp.broadcast_to(every[n:n + 1], (8, batch))

    rows = pl.ds(pl.multiple_of(step * tile, tile), tile)
    k0 = pl.multiple_of(h * key_rows, key_rows)
    a0 = pl.multiple_of(h * 8, 8)

    def lanes_step(c, _):
        lanes = pl.ds(pl.multiple_of(c * LANES, LANES), LANES)
        fade = alpha_t[pl.ds(a0, 8), lanes][0:1]
        new = write_t[rows, lanes]
        keys = key[pl.ds(k0, key_rows), lanes]
        for k in range(key_rows):
            out[k, :, lanes] = fade * state[k, :, lanes] + keys[k:k + 1] * new
        return 0

    lax.fori_loop(0, batch // LANES, lanes_step, 0)


def last_kernel(
    rows, cols, heads,
    recalls, answers, value, gate, scal, head_gain, hid, w_out, final_gain, lm_hbm, tokens, ref_logprob,
    write_g, logprob_out, entropy_out, kl_out,
    lm, token_cols, recall_in, answer_in, w_cols, mixed_g, energy, tall, logits, stats, stats_z,
    lm_sem, rs_send, rs_recv, an_send, an_recv, wo_send, wo_recv, wr_send, wr_recv, mx_send, mx_recv,
    en_send, en_recv, z_send, z_recv, r_send, r_recv, m_send, m_recv, s_send, s_recv, t_send, t_recv,
):
    me_r, me_c, mate = places(rows, cols)
    chips = rows // 2
    count, width = hid.shape
    load = pltpu.make_async_copy(lm_hbm, lm, lm_sem)
    load.start()
    meet(all_peers(rows, cols))
    rs_copies = []
    for step in range(1, cols):
        peer = lax.rem(me_c + step, cols)
        for source, target, send, recv in (
            (recalls, recall_in, rs_send, rs_recv), (answers, answer_in, an_send, an_recv)
        ):
            copy = remote(source.at[peer], target.at[step - 1], send.at[step], recv.at[step], (me_r, peer))
            copy.start()
            rs_copies.append(copy)
    wo_copies = []
    for step in range(1, rows):
        peer = lax.rem(me_r + step, rows)
        columns = pl.ds(pl.multiple_of(peer * width, LANES), width)
        copy = remote(w_out.at[:, columns], w_cols.at[me_r], wo_send.at[step], wo_recv.at[step], (peer, me_c))
        copy.start()
        wo_copies.append(copy)
    w_cols[me_r] = w_out[:, pl.ds(pl.multiple_of(me_r * width, LANES), width)]
    batch = tokens.shape[0]
    for c in range(batch // LANES):
        piece = tokens[c * LANES:(c + 1) * LANES][None, :]
        token_cols[c * LANES:(c + 1) * LANES, :] = jnp.transpose(jnp.broadcast_to(piece, (LANES, LANES)))
    for copy in rs_copies:
        copy.wait_recv()
    total = []
    for source, target in ((recalls, recall_in), (answers, answer_in)):
        part = source[me_c].astype(jnp.float32)
        for step in range(cols - 1):
            part = part + target[step].astype(jnp.float32)
        total.append(part)
    pieces = []
    for h in range(heads):
        span = slice(h * DV, (h + 1) * DV)
        alpha = scal[:, h:h + 1]
        beta = scal[:, heads + h:heads + h + 1]
        inter = scal[:, 2 * heads + h:2 * heads + h + 1]
        write = beta * (value[:, span] - alpha * total[0][:, span])
        write_g[me_c, :, span] = write.astype(jnp.bfloat16)
        readout = alpha * total[1][:, span] + inter * write
        power = jnp.sum(readout * readout, axis=1, keepdims=True)
        gates = gate[:, span]
        silu = gates * (1.0 / (1.0 + jnp.exp(-gates)))
        mixed = readout * lax.rsqrt(power / DV + 1e-05) * head_gain[...][None, :] * silu
        mixed_g[me_r, :, span] = mixed.astype(jnp.bfloat16)
    wr_copies = []
    for step in range(1, cols):
        peer = lax.rem(me_c + step, cols)
        copy = remote(write_g.at[me_c], write_g.at[me_c], wr_send.at[step], wr_recv.at[step], (me_r, peer))
        copy.start()
        wr_copies.append(copy)
    own, copies = row_gather_start(mixed_g, rows, cols, mx_send, mx_recv)
    for copy in wo_copies:
        copy.wait_recv()
    row_gather_finish(mixed_g, rows, cols, mx_send, mx_recv, own, copies)
    hidden = hid[...].astype(jnp.float32)
    branch = jnp.zeros((count, width), jnp.float32)
    for r in range(rows):
        branch = branch + jnp.dot(mixed_g[r], w_cols[r], preferred_element_type=jnp.float32)
    hidden = hidden + branch
    own_energy = jnp.broadcast_to(jnp.sum(hidden * hidden, axis=1, keepdims=True), (count, LANES))
    energy[me_r] = jnp.transpose(own_energy)[0:8, :]
    en_copies = []
    for step in range(1, rows):
        peer = lax.rem(me_r + step, rows)
        copy = remote(energy.at[me_r], energy.at[me_r], en_send.at[step], en_recv.at[step], (peer, me_c))
        copy.start()
        en_copies.append(copy)
    for copy in en_copies:
        copy.wait_recv()
    summed = energy[0]
    for r in range(1, rows):
        summed = summed + energy[r]
    spread = jnp.transpose(jnp.concatenate([summed] * (LANES // 8), axis=0))[:, 0:1]
    final = hidden * lax.rsqrt(spread / (rows * width) + 1e-06) * final_gain[...][None, :].astype(jnp.float32)
    tall[me_r, me_c] = final.astype(jnp.bfloat16)

    z_copies, r_copies, m_copies = [], {}, {}

    def hand_on(source_c, place):
        block = tall.at[me_r, source_c]
        for j in range(1, chips):
            peer = lax.rem(me_r + 2 * j, rows)
            copy = remote(block, block, r_send.at[j, place], r_recv.at[j, place], (peer, me_c))
            copy.start()
            r_copies[j, place] = copy

    def to_mate(source_r, source_c, j, place):
        block = tall.at[source_r, source_c]
        copy = remote(block, block, m_send.at[j, place], m_recv.at[j, place], (mate, me_c))
        copy.start()
        m_copies[j, place] = copy

    def column(place):
        return lax.rem(me_c + cols - place, cols)

    for step in range(1, cols):
        peer = lax.rem(me_c + step, cols)
        block = tall.at[me_r, me_c]
        copy = remote(block, block, z_send.at[step], z_recv.at[step], (me_r, peer))
        copy.start()
        z_copies.append(copy)
    hand_on(me_c, 0)
    to_mate(me_r, me_c, 0, 0)
    for copy in wr_copies:
        copy.wait_recv()
    for place in range(1, cols):
        z_copies[place - 1].wait_recv()
        hand_on(column(place), place)
        to_mate(me_r, column(place), 0, place)
    load.wait()

    def multiply(r, first):
        block = lm[pl.ds(pl.multiple_of(r * width, width), width), :]

        def one(c, _):
            product = jnp.dot(tall[r, c], block, preferred_element_type=jnp.float32)
            logits[c] = product if first else logits[c] + product
            return 0

        lax.fori_loop(0, cols, one, 0)

    multiply(me_r, True)
    for place in range(cols):
        m_copies[0, place].wait_recv()
    multiply(mate, False)
    for j in range(1, chips):
        source = lax.rem(me_r + rows - 2 * j, rows)
        for place in range(cols):
            r_copies[j, place].wait_recv()
            to_mate(source, column(place), j, place)
        multiply(source, False)
        for place in range(cols):
            m_copies[j, place].wait_recv()
        multiply(lax.rem(mate + rows - 2 * j, rows), False)

    vocab = lm.shape[1]
    vocab_start = (me_r * cols + me_c) * vocab
    turned = []
    for c in range(cols):
        part = logits[c]
        at = lax.broadcasted_iota(jnp.int32, part.shape, 1) + vocab_start
        hits = at == token_cols[c * count:(c + 1) * count, 0:1]
        pick = jnp.sum(jnp.where(hits, part, 0.0), axis=1, keepdims=True)
        top = jnp.max(part, axis=1, keepdims=True)
        expo = jnp.exp(part - top)
        mass = jnp.sum(expo, axis=1, keepdims=True)
        weighted = jnp.sum(expo * part, axis=1, keepdims=True)
        lane = lax.broadcasted_iota(jnp.int32, (count, LANES), 1)
        cell = jnp.where(lane == 0, top, jnp.where(lane == 1, mass, jnp.where(lane == 2, weighted, pick)))
        turned.append(jnp.transpose(cell)[0:4, :])
    stats[me_r] = jnp.concatenate(turned, axis=1)

    def merge(slots, number):
        top = slots[0, 0:1, :]
        for n in range(1, number):
            top = jnp.maximum(top, slots[n, 0:1, :])
        mass = jnp.zeros_like(top)
        weighted = jnp.zeros_like(top)
        pick = jnp.zeros_like(top)
        for n in range(number):
            shrink = jnp.exp(slots[n, 0:1, :] - top)
            mass = mass + slots[n, 1:2, :] * shrink
            weighted = weighted + slots[n, 2:3, :] * shrink
            pick = pick + slots[n, 3:4, :]
        return top, mass, weighted, pick

    s_copies = []
    for step in range(1, rows):
        peer = lax.rem(me_r + step, rows)
        copy = remote(stats.at[me_r], stats.at[me_r], s_send.at[step], s_recv.at[step], (peer, me_c))
        copy.start()
        s_copies.append(copy)
    for copy in s_copies:
        copy.wait_recv()
    stats_z[me_c] = jnp.concatenate(merge(stats, rows), axis=0)
    t_copies = []
    for step in range(1, cols):
        peer = lax.rem(me_c + step, cols)
        copy = remote(stats_z.at[me_c], stats_z.at[me_c], t_send.at[step], t_recv.at[step], (me_r, peer))
        copy.start()
        t_copies.append(copy)
    for copy in t_copies:
        copy.wait_recv()
    top, mass, weighted, pick = merge(stats_z, cols)
    lse = top + jnp.log(mass)
    logprob = pick - lse
    logprob_out[...] = logprob.reshape(batch)
    entropy_out[...] = (lse - weighted / mass).reshape(batch)
    gap = jnp.clip(ref_logprob[...][None, :] - logprob, -20.0, 20.0)
    kl_out[...] = jnp.minimum(jnp.exp(gap) - gap - 1.0, 10.0).reshape(batch)
    for copy in rs_copies + wo_copies + wr_copies + en_copies + z_copies + s_copies + t_copies:
        copy.wait_send()
    for copy in list(r_copies.values()) + list(m_copies.values()):
        copy.wait_send()


def fused_device(
    hidden_in, state, attn_norm_gain, w_query, w_key, w_value, w_gate, w_decay, w_beta, decay_log,
    decay_bias, head_gain, w_out, final_gain, lm_weight, token_ids, ref_logprob,
):
    rows = lax.axis_size("row")
    cols = lax.axis_size("col")
    heads = HEADS // rows
    count, width = hidden_in.shape
    key_rows, value_cols, batch = state.shape
    vocab = lm_weight.shape[1]
    line = 2 * heads * key_rows
    bf16, f32 = jnp.bfloat16, jnp.float32
    vmem = pl.BlockSpec(memory_space=pltpu.VMEM)
    hbm = pl.BlockSpec(memory_space=pl.ANY)
    dma = pltpu.SemaphoreType.DMA
    qk, value, gate, scal, alpha = pl.pallas_call(
        functools.partial(first_kernel, rows, cols, heads, key_rows),
        out_shape=[
            jax.ShapeDtypeStruct((cols, count, line), bf16),
            jax.ShapeDtypeStruct((count, value_cols), f32),
            jax.ShapeDtypeStruct((count, value_cols), f32),
            jax.ShapeDtypeStruct((count, LANES), f32),
            jax.ShapeDtypeStruct((cols, 8, count), f32),
        ],
        in_specs=[vmem, vmem] + [hbm] * 4 + [vmem] * 4,
        out_specs=[vmem] * 5,
        scratch_shapes=[
            pltpu.VMEM((rows, count, width), bf16),
            pltpu.VMEM((count, rows * width), bf16),
            pltpu.VMEM((4,) + w_query.shape, bf16),
            pltpu.VMEM((cols, count, line), bf16),
            dma((4,)), dma((rows,)), dma((rows,)), dma((cols,)), dma((cols,)), dma((cols,)), dma((cols,)),
        ],
        compiler_params=pltpu.CompilerParams(collective_id=0, has_side_effects=True),
        name="first",
    )(
        hidden_in, attn_norm_gain, w_query, w_key, w_value, w_gate, w_decay.T, w_beta.T,
        decay_log[None, :], decay_bias[None, :],
    )
    tile = 32
    steps = value_cols // tile
    block = pl.BlockSpec((key_rows, tile, batch), lambda i: (0, i, 0))
    recalls, answers, key = pl.pallas_call(
        functools.partial(response_kernel, heads, key_rows, tile, cols),
        grid=(steps,),
        out_shape=[
            jax.ShapeDtypeStruct((cols, count, value_cols), bf16),
            jax.ShapeDtypeStruct((cols, count, value_cols), f32),
            jax.ShapeDtypeStruct((heads * key_rows, batch), f32),
        ],
        in_specs=[block, pl.BlockSpec((batch, line), lambda i: (0, 0))],
        out_specs=[
            pl.BlockSpec((cols, count, value_cols), lambda i: (0, 0, 0)),
            pl.BlockSpec((cols, count, value_cols), lambda i: (0, 0, 0)),
            pl.BlockSpec((heads * key_rows, batch), lambda i: (0, 0)),
        ],
        scratch_shapes=[pltpu.VMEM((line, batch), f32), pltpu.VMEM((2, DV, batch), f32)],
        compiler_params=pltpu.CompilerParams(dimension_semantics=("arbitrary",)),
        name="responses",
    )(state, qk.reshape(batch, line))
    write, logprob, entropy, kl = pl.pallas_call(
        functools.partial(last_kernel, rows, cols, heads),
        out_shape=[jax.ShapeDtypeStruct((cols, count, value_cols), bf16)]
        + [jax.ShapeDtypeStruct((batch,), f32)] * 3,
        in_specs=[vmem] * 9 + [hbm] + [vmem] * 2,
        out_specs=[vmem] * 4,
        scratch_shapes=[
            pltpu.VMEM(lm_weight.shape, bf16),
            pltpu.VMEM((batch, LANES), jnp.int32),
            pltpu.VMEM((cols - 1, count, value_cols), bf16),
            pltpu.VMEM((cols - 1, count, value_cols), f32),
            pltpu.VMEM((rows, value_cols, width), bf16),
            pltpu.VMEM((rows, count, value_cols), bf16),
            pltpu.VMEM((rows, 8, count), f32),
            pltpu.VMEM((rows, cols, count, width), bf16),
            pltpu.VMEM((cols, count, vocab), f32),
            pltpu.VMEM((rows, 4, batch), f32),
            pltpu.VMEM((cols, 4, batch), f32),
            dma(()), dma((cols,)), dma((cols,)),
            dma((cols,)), dma((cols,)), dma((rows,)), dma((rows,)), dma((cols,)), dma((cols,)),
            dma((rows,)), dma((rows,)), dma((rows,)), dma((rows,)), dma((cols,)), dma((cols,)),
            dma((rows // 2, cols)), dma((rows // 2, cols)), dma((rows // 2, cols)), dma((rows // 2, cols)),
            dma((rows,)), dma((rows,)), dma((cols,)), dma((cols,)),
        ],
        compiler_params=pltpu.CompilerParams(collective_id=1, has_side_effects=True),
        name="last",
    )(
        recalls, answers, value, gate, scal, head_gain, hidden_in, w_out, final_gain, lm_weight,
        token_ids, ref_logprob,
    )
    new_state = pl.pallas_call(
        functools.partial(update_kernel, heads, key_rows, tile),
        grid=(steps,),
        out_shape=jax.ShapeDtypeStruct(state.shape, f32),
        in_specs=[
            block,
            pl.BlockSpec(key.shape, lambda i: (0, 0)),
            pl.BlockSpec(alpha.shape, lambda i: (0, 0, 0)),
            pl.BlockSpec((batch, value_cols), lambda i: (0, 0)),
        ],
        out_specs=block,
        scratch_shapes=[pltpu.VMEM((value_cols, batch), f32), pltpu.VMEM((8 * heads, batch), f32)],
        compiler_params=pltpu.CompilerParams(dimension_semantics=("arbitrary",)),
        name="update",
    )(state, key, alpha, write.reshape(batch, value_cols))
    return new_state, logprob, entropy, kl


def fits(mesh):
    rows, cols = mesh.shape["row"], mesh.shape["col"]
    if rows % 2 or HEADS % rows or DK % cols:
        return False
    return 2 * (HEADS // rows) * (DK // cols) % LANES == 0


def solution(mesh):
    in_specs = (
        P("col", "row"),
        P("col", "row", None),
        P(),
        P(None, "row"),
        P(None, "row"),
        P(None, "row"),
        P(None, "row"),
        P(),
        P(),
        P(),
        P(),
        P(),
        P("row", None),
        P("row"),
        P(None, ("row", "col")),
        P(),
        P(),
    )
    out_specs = (P("col", "row", None), P(), P(), P())
    return jax.shard_map(
        fused_device if fits(mesh) else per_device, mesh=mesh, in_specs=in_specs, out_specs=out_specs, check_vma=False
    )
```
